32 devices in a mesh: role: 4 (over z), dp: 2 (over x), tp: 4 (over y, core).
Axes of the slice: x: 2, y: 2, z: 4, core: 2. Of those that a mesh axis runs over, the one named last changes fastest.
Arguments:
- activations: bfloat16 [2048, 8192], P(('role', 'dp'), 'tp'), may hold values from -6 to 6
- cotangent: bfloat16 [2048, 14336], P(('role', 'dp'), 'tp'), may hold values from -6 to 6
- block_keep: int32 [8], P(('role', 'dp')), may hold values 0 or 1
- input_factor: float32 [64, 8192], P(('role', 'dp'), 'tp'), may hold values from -0.5 to 0.5
- input_mean: float32 [64, 8192], P(('role', 'dp'), 'tp'), may hold values from -6 to 6
- input_square: float32 [64, 8192], P(('role', 'dp'), 'tp'), may hold values from 0.5 to 4
- output_factor: float32 [64, 14336], P(('role', 'dp'), 'tp'), may hold values from -0.3125 to 0.3125
- output_mean: float32 [64, 14336], P(('role', 'dp'), 'tp'), may hold values from -6 to 6
- output_square: float32 [64, 14336], P(('role', 'dp'), 'tp'), may hold values from 0.5 to 4
- frozen_base_rows: bfloat16 [14336, 8192], P(('dp', 'tp')), may hold values from -0.0625 to 0.0625
- prompts: bfloat16 [1024, 8192], P(('role', 'dp', 'tp')), may hold values from -6 to 6
Outputs:
- updated_input: float32 [64, 8192], P(('role', 'dp'), 'tp')
- updated_output: float32 [64, 14336], P(('role', 'dp'), 'tp')
- mean_input: float32 [64, 8192], P(('role', 'dp'), 'tp')
- mean_output: float32 [64, 14336], P(('role', 'dp'), 'tp')
- square_input: float32 [64, 8192], P(('role', 'dp'), 'tp')
- square_output: float32 [64, 14336], P(('role', 'dp'), 'tp')
- merged_weight_rows: bfloat16 [14336, 8192], P(('dp', 'tp'))
- projected: bfloat16 [14336, 1024], P(('dp', 'tp'), 'role')
The draws below stay inside these ranges and needn't reach their ends.
All inputs are finite; a program needn't handle non-finite values. No bound on the sum of `block_keep` on one device may be relied on, other than what follows from the above.
Results may differ from the reference program's by a relative error of at most 0.006.
Values may be sent and summed in bfloat16 or wider, within the bound.
A program may use at most 128 MiB of HBM per device.

```python
import math
import jax
import jax.numpy as jnp
from jax import lax

D = 8192
FFW = 14336
RANK = 64
ROLLOUT_TOKENS = 256
TOKENS = 2048
BLOCKS = 8
PROMPTS = 1024


def touch_ends(result, key, low, high):
    dims = result.shape
    place = [jax.random.randint(jax.random.fold_in(key, axis), (), 0, dims[axis]) for axis in range(len(dims))]
    result = result.at[tuple(place)].set(low)
    longest = dims.index(max(dims))
    place[longest] = (place[longest] + 1) % dims[longest]
    return result.at[tuple(place)].set(high)


def shard_levels(own_key, shape, cuts, smallest, top_value):
    factor_of, own = 1.0, jax.random.fold_in(own_key, 6)
    for dim, shards_of in cuts:
        draws = jnp.exp(jax.random.uniform(jax.random.fold_in(own, dim), (shards_of,), jnp.float32, smallest / len(cuts), top_value / len(cuts)))
        factor_of = factor_of * jnp.repeat(draws, shape[dim] // shards_of).reshape([-1 if axis == dim else 1 for axis in range(len(shape))])
    return factor_of


def scatter_about(own_key, shape, spread, limit, shards=(), dtype=jnp.bfloat16):
    array = jax.random.normal(own_key, shape, jnp.float32) * spread
    if len(shards) > 0:
        array = shard_levels(own_key, shape, shards, -0.22, 0.18) * array
    return jnp.clip(array, min=-limit, max=limit).astype(dtype)


def setup_inputs(seed: int = 0) -> dict:
    key_of = jax.random.split(jax.random.key(seed), 12)
    return {
        "activations": scatter_about(key_of[0], (TOKENS, D), 1.0, 6.0, ((0, 8), (1, 4))),
        "cotangent": scatter_about(key_of[1], (TOKENS, FFW), 1.0, 6.0, ((0, 8), (1, 4))),
        "block_keep": touch_ends((jax.random.randint(key_of[2], (BLOCKS,), 0, 4) < 3).astype(jnp.int32), jax.random.fold_in(key_of[2], 1), 0, 1),
        "input_factor": scatter_about(key_of[3], (RANK, D), 0.035, 0.5, ((0, 8), (1, 4)), jnp.float32),
        "input_mean": scatter_about(key_of[4], (RANK, D), 1.0, 6.0, ((0, 8), (1, 4)), jnp.float32),
        "input_square": jnp.clip(jnp.exp(math.log(4.0) - 2.0794415 * jax.random.uniform(key_of[5], (RANK, D), jnp.float32) ** shard_levels(key_of[5], (RANK, D), ((0, 8), (1, 4)), -0.2, 0.2)), 0.5, 4.0),
        "output_factor": scatter_about(key_of[6], (RANK, FFW), 0.02, 0.3125, ((0, 8), (1, 4)), jnp.float32),
        "output_mean": scatter_about(key_of[7], (RANK, FFW), 1.0, 6.0, ((0, 8), (1, 4)), jnp.float32),
        "output_square": jnp.clip(jnp.exp(math.log(4.0) - 2.0794415 * jax.random.uniform(key_of[8], (RANK, FFW), jnp.float32) ** shard_levels(key_of[8], (RANK, FFW), ((0, 8), (1, 4)), -0.2, 0.2)), 0.5, 4.0),
        "frozen_base_rows": scatter_about(key_of[9], (FFW, D), D ** -0.5, 0.0625, ((0, 8),)),
        "prompts": scatter_about(key_of[10], (PROMPTS, D), 1.0, 6.0, ((0, 32),)),
    }


adapter_scale = 2.0
learn_rate = 0.004
beta_one = 0.9
beta_two = 0.95
epsilon = 1e-08
first_fix = 1.0 - 0.9 ** 20
second_fix = 1.0 - 0.95 ** 20

def adam_update(factor, moment, square, gradient):
    moment_new = beta_one * moment + (1.0 - beta_one) * gradient
    square_new = beta_two * square + (1.0 - beta_two) * gradient * gradient
    factor_new = factor - learn_rate * (moment_new / first_fix) / (jnp.sqrt(square_new / second_fix) + epsilon)
    return (factor_new, moment_new, square_new)

def masked(values, block_keep):
    blocks = block_keep.shape[0]
    reshaped_rows = values.reshape(blocks, values.shape[0] // blocks, values.shape[1])
    weighted = reshaped_rows * block_keep.astype(jnp.float32)[:, None, None]
    return weighted.reshape(values.shape).astype(jnp.bfloat16)

def contract_rows(left, right):
    return lax.dot_general(left, right, (((0,), (0,)), ((), ())), preferred_element_type=jnp.float32)

def contract_cols(left, right):
    return lax.dot_general(left, right, (((1,), (1,)), ((), ())), preferred_element_type=jnp.float32)

def reference(activations, cotangent, block_keep, input_factor, input_mean, input_square, output_factor, output_mean, output_square, frozen_base_rows, prompts):
    input_rows = input_factor.astype(jnp.bfloat16)
    output_rows = output_factor.astype(jnp.bfloat16)
    low_input = jnp.dot(activations, input_rows.T, preferred_element_type=jnp.float32)
    low_grad = jnp.dot(cotangent, output_rows.T, preferred_element_type=jnp.float32)
    input_kept = masked(low_input, block_keep)
    grad_kept = masked(low_grad, block_keep)
    adapter_factor_scale = adapter_scale / ROLLOUT_TOKENS
    input_grad = contract_rows(grad_kept, activations) * adapter_factor_scale
    output_grad = contract_rows(input_kept, cotangent) * adapter_factor_scale
    input_new, input_moment, input_second = adam_update(input_factor, input_mean, input_square, input_grad)
    output_new, output_moment, output_second = adam_update(output_factor, output_mean, output_square, output_grad)
    adapter_delta_rows = contract_rows(output_new.astype(jnp.bfloat16), input_new.astype(jnp.bfloat16))
    merged_weight_rows = (frozen_base_rows.astype(jnp.float32) + adapter_scale * adapter_delta_rows).astype(jnp.bfloat16)
    projected = contract_cols(merged_weight_rows, prompts).astype(jnp.bfloat16)
    return (input_new, output_new, input_moment, output_moment, input_second, output_second, merged_weight_rows, projected)
```

```python
import functools

import jax
import jax.numpy as jnp
from jax import lax
from jax.experimental import pallas as pl
from jax.experimental.pallas import tpu as pltpu
from jax.sharding import PartitionSpec as P

ROLLOUT_TOKENS = 256


adapter_scale = 2.0
learn_rate = 0.004
beta_one = 0.9
beta_two = 0.95
epsilon = 1e-08
first_fix = 1.0 - 0.9**20
second_fix = 1.0 - 0.95**20


def adam_update(factor, moment, square, gradient):
    moment_new = beta_one * moment + (1.0 - beta_one) * gradient
    square_new = beta_two * square + (1.0 - beta_two) * gradient * gradient
    factor_new = factor - learn_rate * (moment_new / first_fix) / (
        jnp.sqrt(square_new / second_fix) + epsilon
    )
    return (factor_new, moment_new, square_new)


def masked(values, block_keep):
    blocks = block_keep.shape[0]
    reshaped_rows = values.reshape(blocks, values.shape[0] // blocks, values.shape[1])
    weighted = reshaped_rows * block_keep.astype(jnp.float32)[:, None, None]
    return weighted.reshape(values.shape).astype(jnp.bfloat16)


def contract_rows(left, right):
    return lax.dot_general(
        left, right, (((0,), (0,)), ((), ())), preferred_element_type=jnp.float32
    )


def contract_cols(left, right):
    return lax.dot_general(
        left, right, (((1,), (1,)), ((), ())), preferred_element_type=jnp.float32
    )


VMEM = pl.BlockSpec(memory_space=pltpu.VMEM)
MESH = pl.DeviceIdType.MESH


def places():
    return tuple(lax.axis_index(name) for name in ("role", "dp", "tp"))


def sizes():
    return tuple(lax.axis_size(name) for name in ("role", "dp", "tp"))


def enter(peers):
    barrier = pltpu.get_barrier_semaphore()
    for peer in peers:
        pl.semaphore_signal(barrier, inc=1, device_id=peer, device_id_type=MESH)
    pl.semaphore_wait(barrier, len(peers))


def send(source, target, send_sem, recv_sem, peer):
    copy = pltpu.make_async_remote_copy(
        src_ref=source,
        dst_ref=target,
        send_sem=send_sem,
        recv_sem=recv_sem,
        device_id=peer,
        device_id_type=MESH,
    )
    copy.start()
    return copy


def landed(slot, sem):
    pltpu.make_async_copy(slot, slot, sem).wait()


def communicate(kernel, name, outs, scratch, collective_id, args):
    return pl.pallas_call(
        kernel,
        name=name,
        out_shape=outs,
        in_specs=[VMEM] * len(args),
        out_specs=[VMEM] * len(outs),
        scratch_shapes=scratch,
        compiler_params=pltpu.CompilerParams(
            collective_id=collective_id,
            has_side_effects=True,
            vmem_limit_bytes=40 * 1024 * 1024,
        ),
        cost_estimate=pl.CostEstimate(
            flops=10**9, bytes_accessed=10**7, transcendentals=0
        ),
    )(*args)


def dma(*shape):
    return pltpu.SemaphoreType.DMA(shape)


def gather_kernel(count, *refs):
    ins, outs = refs[:count], refs[count : 2 * count]
    own, send_role, recv_role, send_dp, recv_dp = refs[2 * count :]
    role, dp, tp = places()
    roles, dps, _ = sizes()
    role_peers = [(lax.rem(role + k, roles), dp, tp) for k in range(1, roles)]
    dp_peers = [(role, lax.rem(dp + j, dps), tp) for j in range(1, dps)]
    enter(role_peers + dp_peers)
    copies = []
    for i in range(count):
        for k in range(1, roles):
            copies.append(send(ins[i], outs[i].at[dp, role], send_role.at[i, k], recv_role.at[i, k], role_peers[k - 1]))
        for j in range(1, dps):
            copies.append(send(ins[i], outs[i].at[dp, role], send_dp.at[i, j, 0], recv_dp.at[i, j, 0], dp_peers[j - 1]))
        local = pltpu.make_async_copy(ins[i], outs[i].at[dp, role], own.at[i])
        local.start()
    for i in range(count):
        for k in range(1, roles):
            slot = outs[i].at[dp, lax.rem(role + roles - k, roles)]
            landed(slot, recv_role.at[i, k])
            for j in range(1, dps):
                copies.append(send(slot, slot, send_dp.at[i, j, k], recv_dp.at[i, j, k], dp_peers[j - 1]))
    for i in range(count):
        pltpu.make_async_copy(ins[i], outs[i].at[dp, role], own.at[i]).wait()
        for j in range(1, dps):
            for k in range(roles):
                slot = outs[i].at[lax.rem(dp + dps - j, dps), lax.rem(role + roles - k, roles)]
                landed(slot, recv_dp.at[i, j, k])
    for copy in copies:
        copy.wait_send()


def gather_rows(arrays):
    roles, dps, _ = sizes()
    n = len(arrays)
    return communicate(
        functools.partial(gather_kernel, n),
        "gather_rows",
        [jax.ShapeDtypeStruct((dps, roles, *x.shape), x.dtype) for x in arrays],
        [dma(n), dma(n, roles), dma(n, roles), dma(n, dps, roles), dma(n, dps, roles)],
        0,
        arrays,
    )


def features_kernel(count, *refs):
    ins, outs = refs[:count], refs[count : 2 * count]
    slots = refs[2 * count : 3 * count]
    sends, recvs = refs[3 * count :]
    role, dp, tp = places()
    tps = sizes()[2]
    peers = [(role, dp, lax.rem(tp + k, tps)) for k in range(1, tps)]
    enter(peers)
    copies = []
    for i in range(count):
        for k in range(1, tps):
            copies.append(send(ins[i], slots[i].at[k - 1], sends.at[i, k], recvs.at[i, k], peers[k - 1]))
    for i in range(count):
        total = ins[i][...]
        for k in range(1, tps):
            landed(slots[i].at[k - 1], recvs.at[i, k])
            total = total + slots[i][k - 1]
        outs[i][...] = total
    for copy in copies:
        copy.wait_send()


def sum_features(arrays):
    tps = sizes()[2]
    n = len(arrays)
    return communicate(
        functools.partial(features_kernel, n),
        "sum_features",
        [jax.ShapeDtypeStruct(x.shape, x.dtype) for x in arrays],
        [pltpu.VMEM((max(tps - 1, 1), *x.shape), x.dtype) for x in arrays] + [dma(n, tps), dma(n, tps)],
        1,
        arrays,
    )


def tokens_kernel(count, *refs):
    ins, outs = refs[:count], refs[count : 2 * count]
    slots = refs[2 * count : 3 * count]
    sends, recvs = refs[3 * count :]
    role, dp, tp = places()
    roles, dps, _ = sizes()
    offsets = [(j, k) for k in range(roles) for j in range(dps) if (j, k) != (0, 0)]
    offsets.sort(key=lambda o: -min(o[1], roles - o[1]))
    peers = {(j, k): (lax.rem(role + k, roles), lax.rem(dp + j, dps), tp) for j, k in offsets}
    enter(list(peers.values()))
    copies = []
    for i in range(count):
        for j, k in offsets:
            peer = peers[j, k]
            copies.append(send(ins[i].at[peer[1], peer[0]], slots[i].at[j, k], sends.at[i, j, k], recvs.at[i, j, k], peer))
    for i in range(count):
        total = ins[i][dp, role].astype(jnp.float32)
        for j, k in reversed(offsets):
            landed(slots[i].at[j, k], recvs.at[i, j, k])
            total = total + slots[i][j, k].astype(jnp.float32)
        outs[i][...] = total
    for copy in copies:
        copy.wait_send()


def sum_tokens(arrays):
    roles, dps, _ = sizes()
    n = len(arrays)
    return communicate(
        functools.partial(tokens_kernel, n),
        "sum_tokens",
        [jax.ShapeDtypeStruct(x.shape[2:], jnp.float32) for x in arrays],
        [pltpu.VMEM(x.shape, x.dtype) for x in arrays] + [dma(n, dps, roles), dma(n, dps, roles)],
        2,
        arrays,
    )


def spread_kernel(a_ref, b_ref, whole_ref, slice_ref, own, send_b, recv_b, send_role, recv_role, send_dp, recv_dp, send_hi, recv_hi, send_lo, recv_lo):
    role, dp, tp = places()
    roles, dps, tps = sizes()
    half = tps // 2
    devices = roles * dps * tps
    me = (role * dps + dp) * tps + tp

    barrier = pltpu.get_barrier_semaphore()

    @pl.loop(1, devices)
    def _(step):
        other = lax.rem(me + step, devices)
        peer = (other // (dps * tps), lax.rem(other // tps, dps), lax.rem(other, tps))
        pl.semaphore_signal(barrier, inc=1, device_id=peer, device_id_type=MESH)

    pl.semaphore_wait(barrier, devices - 1)

    role_peers = [(lax.rem(role + k, roles), dp, tp) for k in range(1, roles)]
    dp_peers = [(role, lax.rem(dp + j, dps), tp) for j in range(1, dps)]
    hi_peers = [(role, dp, lax.rem(tp + 2 * h, tps)) for h in range(1, half)]
    lo_peer = (role, dp, tp + 1 - 2 * lax.rem(tp, 2))

    home = whole_ref.at[tp, dp, role]
    copies = []
    for k in range(1, roles):
        copies.append(send(a_ref, home, send_role.at[k], recv_role.at[k], role_peers[k - 1]))
    for j in range(1, dps):
        copies.append(send(a_ref, home, send_dp.at[j, 0], recv_dp.at[j, 0], dp_peers[j - 1]))
    local = pltpu.make_async_copy(a_ref, home, own.at[0])
    local.start()

    def b_copy(i, k):
        block = tp * dps + i
        peer = (lax.rem(role + k, roles), block // tps, lax.rem(block, tps))
        place = slice_ref.at[dp, role]
        remote = pltpu.make_async_remote_copy(
            src_ref=b_ref.at[i], dst_ref=place, send_sem=send_b.at[i, k], recv_sem=recv_b.at[dp, role],
            device_id=peer, device_id_type=MESH,
        )
        if k > 0:
            return None, remote, None
        here = (block // tps == dp) & (lax.rem(block, tps) == tp)
        return here, remote, pltpu.make_async_copy(b_ref.at[i], place, recv_b.at[dp, role])

    for k in range(roles):
        for i in range(dps):
            here, remote, beside = b_copy(i, k)
            if here is None:
                remote.start()
            else:
                pl.when(here)(beside.start)
                pl.when(jnp.logical_not(here))(remote.start)

    for k in range(1, roles):
        slot = whole_ref.at[tp, dp, lax.rem(role + roles - k, roles)]
        landed(slot, recv_role.at[k])
        for j in range(1, dps):
            copies.append(send(slot, slot, send_dp.at[j, k], recv_dp.at[j, k], dp_peers[j - 1]))
    local.wait()
    for j in range(dps):
        from_dp = lax.rem(dp + dps - j, dps)
        if j > 0:
            for k in range(roles):
                landed(whole_ref.at[tp, from_dp, lax.rem(role + roles - k, roles)], recv_dp.at[j, k])
        group = whole_ref.at[tp, from_dp]
        for h in range(1, half):
            copies.append(send(group, group, send_hi.at[h, j], recv_hi.at[h, j], hi_peers[h - 1]))
        copies.append(send(group, group, send_lo.at[0, j], recv_lo.at[0, j], lo_peer))
    for j in range(dps):
        from_dp = lax.rem(dp + dps - j, dps)
        for h in range(1, half):
            group = whole_ref.at[lax.rem(tp + tps - 2 * h, tps), from_dp]
            landed(group, recv_hi.at[h, j])
            copies.append(send(group, group, send_lo.at[h, j], recv_lo.at[h, j], lo_peer))
    other = lo_peer[2]
    for j in range(dps):
        from_dp = lax.rem(dp + dps - j, dps)
        for h in range(half):
            landed(whole_ref.at[lax.rem(other + tps - 2 * h, tps), from_dp], recv_lo.at[h, j])
    for d in range(dps):
        for r in range(roles):
            landed(slice_ref.at[d, r], recv_b.at[d, r])
    for k in range(roles):
        for i in range(dps):
            here, remote, _ = b_copy(i, k)
            if here is None:
                remote.wait_send()
            else:
                pl.when(jnp.logical_not(here))(remote.wait_send)
    for copy in copies:
        copy.wait_send()


def spread(a, b):
    roles, dps, tps = sizes()
    half = max(tps // 2, 1)
    return communicate(
        spread_kernel,
        "spread",
        [
            jax.ShapeDtypeStruct((tps, dps, roles, *a.shape), a.dtype),
            jax.ShapeDtypeStruct((dps, roles, *b.shape[1:]), b.dtype),
        ],
        [
            dma(1), dma(dps, roles), dma(dps, roles), dma(roles), dma(roles),
            dma(dps, roles), dma(dps, roles), dma(half, dps), dma(half, dps), dma(half, dps), dma(half, dps),
        ],
        3,
        [a, b],
    )


def merge_kernel(base_ref, b_ref, a_ref, prompts_ref, merged_ref, projected_ref):
    shards, _, width = a_ref.shape
    total = jnp.zeros(projected_ref.shape, jnp.float32)
    for shard in range(shards):
        columns = pl.ds(shard * width, width)
        delta = jnp.dot(b_ref[...], a_ref[shard], preferred_element_type=jnp.float32)
        merged = (base_ref[:, columns].astype(jnp.float32) + adapter_scale * delta).astype(jnp.bfloat16)
        merged_ref[:, columns] = merged
        total = total + contract_cols(merged, prompts_ref[:, columns])
    projected_ref[...] = total.astype(projected_ref.dtype)


def merge(base, b, a, prompts):
    rows, width = base.shape
    tile = max(t for t in range(16, 257, 16) if rows % t == 0)
    count = prompts.shape[0]
    return pl.pallas_call(
        merge_kernel,
        name="merge",
        grid=(rows // tile,),
        out_shape=[
            jax.ShapeDtypeStruct(base.shape, base.dtype),
            jax.ShapeDtypeStruct((rows, count), jnp.bfloat16),
        ],
        in_specs=[
            pl.BlockSpec((tile, width), lambda i: (i, 0)),
            pl.BlockSpec((tile, b.shape[1]), lambda i: (i, 0)),
            VMEM,
            VMEM,
        ],
        out_specs=[
            pl.BlockSpec((tile, width), lambda i: (i, 0)),
            pl.BlockSpec((tile, count), lambda i: (i, 0)),
        ],
        compiler_params=pltpu.CompilerParams(vmem_limit_bytes=56 * 1024 * 1024),
        cost_estimate=pl.CostEstimate(
            flops=2 * rows * width * (count + b.shape[1]), bytes_accessed=4 * rows * width, transcendentals=0
        ),
    )(base, b, a, prompts)


def body(
    activations,
    cotangent,
    block_keep,
    input_factor,
    input_mean,
    input_square,
    output_factor,
    output_mean,
    output_square,
    frozen_base_rows,
    prompts,
):
    roles, dps, tps = sizes()
    rows = input_factor.shape[0]
    rank = roles * dps * rows
    group_prompts = lax.all_gather(prompts, ("dp", "tp"), axis=0, tiled=True)
    input_rows, output_rows = gather_rows(
        [input_factor.astype(jnp.bfloat16), output_factor.astype(jnp.bfloat16)]
    )
    low_input = contract_cols(activations, input_rows.reshape(rank, -1))
    low_grad = contract_cols(cotangent, output_rows.reshape(rank, -1))
    low_input, low_grad = sum_features([low_input, low_grad])
    input_kept = masked(low_input, block_keep)
    grad_kept = masked(low_grad, block_keep)
    input_part = contract_rows(grad_kept, activations).astype(jnp.bfloat16)
    output_part = contract_rows(input_kept, cotangent).astype(jnp.bfloat16)
    input_sum, output_sum = sum_tokens(
        [part.reshape(dps, roles, rows, -1) for part in (input_part, output_part)]
    )
    adapter_factor_scale = adapter_scale / ROLLOUT_TOKENS
    input_new, input_moment, input_second = adam_update(
        input_factor, input_mean, input_square, input_sum * adapter_factor_scale
    )
    output_new, output_moment, output_second = adam_update(
        output_factor, output_mean, output_square, output_sum * adapter_factor_scale
    )
    input_send = input_new.astype(jnp.bfloat16)
    output_send = output_new.astype(jnp.bfloat16).reshape(rows, dps, -1).swapaxes(0, 1)
    input_whole, output_slice = spread(input_send, output_send)
    merged_weight_rows, projected = merge(
        frozen_base_rows,
        output_slice.reshape(rank, -1).T,
        input_whole.reshape(tps, rank, -1),
        group_prompts,
    )
    return (
        input_new,
        output_new,
        input_moment,
        output_moment,
        input_second,
        output_second,
        merged_weight_rows,
        projected,
    )


def solution(mesh):
    placed = (
        P(("role", "dp"), "tp"),
        P(("role", "dp"), "tp"),
        P(("role", "dp")),
        P(("role", "dp"), "tp"),
        P(("role", "dp"), "tp"),
        P(("role", "dp"), "tp"),
        P(("role", "dp"), "tp"),
        P(("role", "dp"), "tp"),
        P(("role", "dp"), "tp"),
        P(("dp", "tp"), None),
        P(("role", "dp", "tp"), None),
    )
    return jax.shard_map(
        body,
        mesh=mesh,
        in_specs=placed,
        out_specs=(
            P(("role", "dp"), "tp"),
            P(("role", "dp"), "tp"),
            P(("role", "dp"), "tp"),
            P(("role", "dp"), "tp"),
            P(("role", "dp"), "tp"),
            P(("role", "dp"), "tp"),
            P(("dp", "tp"), None),
            P(("dp", "tp"), "role"),
        ),
        check_vma=False,
    )
```
